32 devices in a mesh: section: 4 (over z), tp: 8 (over y, x, core).
Axes of the slice: x: 2, y: 2, z: 4, core: 2. Of those that a mesh axis runs over, the one named last changes fastest.
Arguments:
- latents: bfloat16 [1024, 8, 2048], P('tp', 'section'), may hold values from -6 to 6
- timestep: int32 [8], replicated, may hold values from 0 to 999
- target: int32 [8], replicated, may hold values from 0 to 3, as said below
- qkv_weight: bfloat16 [4, 2048, 3, 2048], P('section', None, None, 'tp'), may hold values from -0.125 to 0.125
- mod_weight: bfloat16 [4, 256, 3, 2048], P('section'), may hold values from -2.6 to 2.6
- out_weight: bfloat16 [4, 2048, 2048], P('section', 'tp'), may hold values from -0.125 to 0.125
Outputs:
- updated: bfloat16 [1024, 8, 2048], P('tp', 'section')
The draws below stay inside these ranges and needn't reach their ends.
Inputs may be any that keep to these rules, and one draw needn't show every extreme that they name: target[l] is l // 2 or l // 2 + 1; of one section's 2 latents at most 1 name the next section, exactly 1 for section 0, none for the last section.
All inputs are finite; a program needn't handle non-finite values.
Results may differ from the reference program's by a relative error of at most 0.023.
Values may be sent and summed in bfloat16 or wider, within the bound.
No kernel may reach another device: no remote copies, remote signals or barrier semaphores. Data moves between devices by JAX's collectives and lax.ppermute only.
A program may use at most 128 MiB of HBM per device.

```python
import math
import jax
import jax.numpy as jnp
from jax import lax

D = 2048
HEADS = 16
HEAD_DIM = 128
FREQ = 256
TOK = 1024
LAT_SECTION = 2
MOVE_MAX = 1
SECTIONS = 4
LATENTS = 8
N_TP = 8


def draw_target(key, part):
    counts = jax.random.randint(jax.random.fold_in(key, 11), (SECTIONS,), 0, MOVE_MAX + 1)
    section_ids = jnp.arange(SECTIONS, dtype=jnp.int32)
    counts = jnp.where(section_ids == 0, MOVE_MAX, counts)
    counts = jnp.where(section_ids == SECTIONS - 1, 0, counts)
    row_keys = jax.random.split(jax.random.fold_in(key, 12), SECTIONS)
    ranks = jax.vmap(lambda row_key: jax.random.permutation(row_key, LAT_SECTION))(row_keys)
    movers = (ranks < counts[:, None]).astype(jnp.int32)
    return (section_ids[:, None] + movers).reshape(LATENTS).astype(jnp.int32)


def draw_mod_weight(key, part):
    base = jnp.clip(jax.random.normal(jax.random.fold_in(key, 21), (SECTIONS, FREQ, 3, D), jnp.float32), -4.0, 4.0)
    return (base * 0.2).astype(jnp.bfloat16)


def with_ends(result, rng, low, largest):
    place = [jax.random.randint(jax.random.fold_in(rng, axis), (), 0, length) for axis, length in enumerate(result.shape)]
    main_axis = result.shape.index(max(result.shape))
    next_to = place[:main_axis] + [(place[main_axis] + 1) % result.shape[main_axis]] + place[main_axis + 1:]
    return result.at[tuple(place)].set(low).at[tuple(next_to)].set(largest)


def level_of(key, extent, cuts, low, high):
    def one(position, blocks):
        heights = jax.random.uniform(jax.random.fold_in(jax.random.fold_in(key, 6), position), (blocks,), jnp.float32, low / len(cuts), high / len(cuts))
        return jnp.repeat(jnp.exp(heights), extent[position] // blocks).reshape((-1,) + (1,) * (len(extent) - position - 1))

    gain = one(*cuts[0])
    for cut in cuts[1:]:
        gain = gain * one(*cut)
    return gain


def scatter_about(own_key, extent, spread, limit, pieces=(), kind=jnp.bfloat16):
    result = jax.random.normal(own_key, extent, jnp.float32) * spread
    if len(pieces) > 0:
        result = level_of(own_key, extent, pieces, -0.22, 0.18) * result
    return jnp.clip(result, min=-limit, max=limit).astype(kind)


def setup_inputs(seed: int = 0) -> dict:
    seeds = jax.random.split(jax.random.key(seed), 7)
    return {
        "latents": scatter_about(seeds[0], (TOK, LATENTS, D), 1.0, 6.0, ((0, 8), (1, 4))),
        "timestep": with_ends(jax.random.randint(seeds[1], (LATENTS,), 0, 1000), jax.random.fold_in(seeds[1], 1), 0, 999).astype(jnp.int32),
        "target": draw_target(jax.random.fold_in(seeds[6], 71), 0),
        "qkv_weight": scatter_about(seeds[3], (SECTIONS, D, 3, D), D ** -0.5, 0.125, ((0, 4), (3, 8))),
        "mod_weight": draw_mod_weight(jax.random.fold_in(seeds[6], 71), 0),
        "out_weight": scatter_about(seeds[5], (SECTIONS, D, D), D ** -0.5, 0.125, ((0, 4), (1, 8))),
    }


def time_embed(steps):
    half_width = FREQ // 2
    frequency = jnp.exp(-math.log(10000.0) * jnp.arange(half_width, dtype=jnp.float32) / half_width)
    angles = steps.astype(jnp.float32)[:, None] * frequency[None, :]
    return jnp.concatenate([jnp.cos(angles), jnp.sin(angles)], axis=1)

def modulate(steps, mod_table):
    feature = jax.nn.silu(time_embed(steps))
    return jnp.einsum('bf,fcd->bcd', feature, mod_table.astype(jnp.float32), precision=lax.Precision.HIGHEST)

def normalize(values, shift, scale):
    row_mean = lax.optimization_barrier(jnp.mean(values, axis=-1, keepdims=True))
    centred = values - row_mean
    variance = lax.optimization_barrier(jnp.mean(centred * centred, axis=-1, keepdims=True))
    return centred * lax.rsqrt(variance + 1e-06) * (1.0 + scale) + shift

def reference(latents, timestep, target, qkv_weight, mod_weight, out_weight):

    def one_latent(index):
        tokens = lax.dynamic_index_in_dim(latents, index, 1, keepdims=False)
        section_id = lax.dynamic_index_in_dim(target, index, 0, keepdims=False)
        step_now = lax.dynamic_slice_in_dim(timestep, index, 1)
        table = lax.dynamic_index_in_dim(mod_weight, section_id, 0, keepdims=False)
        qkv_table = lax.dynamic_index_in_dim(qkv_weight, section_id, 0, keepdims=False)
        out_table = lax.dynamic_index_in_dim(out_weight, section_id, 0, keepdims=False)
        mods = modulate(step_now, table)[0]
        values = tokens.astype(jnp.float32)
        hidden = normalize(values, mods[0], mods[1]).astype(jnp.bfloat16)
        packed = jnp.dot(hidden, qkv_table.reshape(D, 3 * D), preferred_element_type=jnp.float32)
        packed = packed.astype(jnp.bfloat16).reshape(TOK, 3, HEADS, HEAD_DIM)
        query = packed[:, 0].astype(jnp.float32)
        keys = packed[:, 1].astype(jnp.float32)
        vals = packed[:, 2].astype(jnp.float32)
        scores = jnp.einsum('qhe,khe->hqk', query, keys) * HEAD_DIM ** (-0.5)
        soft = jax.nn.softmax(scores, axis=-1).astype(jnp.bfloat16)
        mixed = jnp.einsum('hqk,khe->qhe', soft.astype(jnp.float32), vals).astype(jnp.bfloat16)
        grouped = mixed.reshape(TOK, N_TP, D // N_TP).astype(jnp.float32)
        out_groups = out_table.reshape(N_TP, D // N_TP, D).astype(jnp.float32)
        partial_terms = jnp.einsum('sgk,gkd->gsd', grouped, out_groups).astype(jnp.bfloat16)
        partial_terms = lax.optimization_barrier(partial_terms)
        proj = lax.optimization_barrier(jnp.sum(partial_terms.astype(jnp.float32), axis=0))
        return (values + mods[2] * proj).astype(jnp.bfloat16)
    results = lax.map(one_latent, jnp.arange(LATENTS, dtype=jnp.int32))
    return jnp.moveaxis(results, 0, 1)
```

```python
import functools
import math

import jax
import jax.numpy as jnp
from jax import lax
from jax.experimental import pallas as pl
from jax.experimental.pallas import tpu as pltpu
from jax.sharding import PartitionSpec as P

HEAD_DIM = 128
FREQ = 256


def time_embed(steps):
    half_width = FREQ // 2
    frequency = jnp.exp(-math.log(10000.0) * jnp.arange(half_width, dtype=jnp.float32) / half_width)
    angles = steps.astype(jnp.float32)[:, None] * frequency[None, :]
    return jnp.concatenate([jnp.cos(angles), jnp.sin(angles)], axis=1)


def modulate(steps, mod_table):
    feature = jax.nn.silu(time_embed(steps))
    return jnp.einsum(
        "bf,fcd->bcd", feature, mod_table.astype(jnp.float32), precision=lax.Precision.HIGHEST
    )


def normalize(values, shift, scale):
    row_mean = jnp.mean(values, axis=-1, keepdims=True)
    centred = values - row_mean
    variance = jnp.mean(centred * centred, axis=-1, keepdims=True)
    return centred * lax.rsqrt(variance + 1e-06) * (1.0 + scale) + shift


def from_behind(shard, axis, by):
    peers = lax.axis_size(axis)
    pairs = [(i, i + by) for i in range(peers) if 0 <= i + by < peers]
    return lax.ppermute(shard, axis, pairs)


def swap(shard, mask):
    return lax.ppermute(shard, "tp", [(i, i ^ mask) for i in range(lax.axis_size("tp"))])


def chip_masks():
    return tuple(range(0, lax.axis_size("tp"), 2))


def gather_even(shard, axis):
    masks = chip_masks()
    if len(masks) != 4:
        return [[shard] if m == 0 else [swap(shard, m)] for m in masks]
    half = shard.shape[axis] // 2
    from_x = swap(shard, 2)
    from_y = swap(shard, 4)
    far_low = swap(lax.slice_in_dim(from_y, 0, half, axis=axis), 2)
    far_high = swap(lax.slice_in_dim(from_x, half, 2 * half, axis=axis), 4)
    return [[shard], [from_x], [from_y], [far_low, far_high]]


def qkv_kernel(*refs, n_pieces):
    pieces = refs[:n_pieces]
    w_own, w_peer, out_own, out_peer, tokens = refs[n_pieces:]
    at = 0
    for piece in pieces:
        rows = piece.shape[1]
        tokens[at : at + rows, :] = piece[0]
        at += rows
    block = tokens[...]
    out_own[0] = jnp.dot(block, w_own[...], preferred_element_type=jnp.float32).astype(jnp.bfloat16)
    out_peer[0] = jnp.dot(block, w_peer[...], preferred_element_type=jnp.float32).astype(jnp.bfloat16)


def project_qkv(pieces, w_own, w_peer):
    flat = [p for group in pieces for p in group]
    slots, _, width = flat[0].shape
    rows = sum(p.shape[1] for p in flat)
    cols = w_own.shape[1]
    shape = jax.ShapeDtypeStruct((slots, rows, cols), jnp.bfloat16)
    return pl.pallas_call(
        functools.partial(qkv_kernel, n_pieces=len(flat)),
        grid=(slots,),
        in_specs=[pl.BlockSpec((1, p.shape[1], width), lambda i: (i, 0, 0)) for p in flat]
        + [pl.BlockSpec((width, cols), lambda i: (0, 0))] * 2,
        out_specs=[pl.BlockSpec((1, rows, cols), lambda i: (i, 0, 0))] * 2,
        out_shape=[shape, shape],
        scratch_shapes=[pltpu.VMEM((rows, width), jnp.bfloat16)],
        cost_estimate=pl.CostEstimate(
            flops=4 * slots * rows * width * cols,
            transcendentals=0,
            bytes_accessed=4 * width * cols + 2 * slots * rows * (width + 2 * cols),
        ),
        name="qkv",
    )(*flat, w_own, w_peer)


def attention_kernel(own, peer, *outs, tok):
    heads = own.shape[2] // (3 * HEAD_DIM)
    width = heads * HEAD_DIM
    factor = HEAD_DIM ** (-0.5) * math.log2(math.e)
    for h in range(heads):
        cols = lambda part: slice(part * width + h * HEAD_DIM, part * width + (h + 1) * HEAD_DIM)
        keys = jnp.concatenate([own[0, :, cols(1)], peer[0, :, cols(1)]], axis=0)
        vals = jnp.concatenate([own[0, :, cols(2)], peer[0, :, cols(2)]], axis=0)
        for m, out in enumerate(outs):
            query = jnp.concatenate(
                [own[0, m * tok : (m + 1) * tok, cols(0)], peer[0, m * tok : (m + 1) * tok, cols(0)]],
                axis=0,
            )
            scores = lax.dot_general(
                query, keys, (((1,), (1,)), ((), ())), preferred_element_type=jnp.float32
            )
            top = jnp.max(scores, axis=1, keepdims=True)
            soft = jnp.exp2((scores - top) * factor)
            total = jnp.sum(soft, axis=1, keepdims=True)
            mixed = jnp.dot(soft.astype(jnp.bfloat16), vals, preferred_element_type=jnp.float32)
            out[0, :, h * HEAD_DIM : (h + 1) * HEAD_DIM] = (mixed / total).astype(jnp.bfloat16)


def attend(own, peer, tok):
    slots, rows, cols = own.shape
    n_out = rows // tok
    spec = pl.BlockSpec((1, rows, cols), lambda i: (i, 0, 0))
    shape = jax.ShapeDtypeStruct((slots, 2 * tok, cols // 3), jnp.bfloat16)
    pairs = slots * (cols // (3 * HEAD_DIM)) * 4 * rows * rows
    return pl.pallas_call(
        functools.partial(attention_kernel, tok=tok),
        grid=(slots,),
        in_specs=[spec, spec],
        out_specs=[pl.BlockSpec((1, 2 * tok, cols // 3), lambda i: (i, 0, 0))] * n_out,
        out_shape=[shape] * n_out,
        cost_estimate=pl.CostEstimate(
            flops=4 * pairs * HEAD_DIM,
            transcendentals=pairs,
            bytes_accessed=6 * slots * rows * cols,
        ),
        name="attend",
    )(own, peer)


def project_kernel(*refs, n_mixed, n_weight):
    mixed = refs[:n_mixed]
    weights = refs[n_mixed : n_mixed + n_weight]
    out_own, out_peer, table, packed = refs[n_mixed + n_weight :]

    @pl.when(pl.program_id(0) == 0)
    def _():
        at = 0
        for w in weights:
            table[at : at + w.shape[0], :] = w[...]
            at += w.shape[0]

    for m, block in enumerate(mixed):
        width = block.shape[2]
        packed[:, m * width : (m + 1) * width] = block[0]
    proj = jnp.dot(packed[...], table[...], preferred_element_type=jnp.float32)
    tok = out_own.shape[1]
    out_own[0] = proj[:tok]
    out_peer[0] = proj[tok:].astype(jnp.bfloat16)


def project_out(mixed, weights):
    flat = [w for group in weights for w in group]
    slots, rows, width = mixed[0].shape
    depth = sum(w.shape[0] for w in flat)
    cols = flat[0].shape[1]
    tok = rows // 2
    return pl.pallas_call(
        functools.partial(project_kernel, n_mixed=len(mixed), n_weight=len(flat)),
        grid=(slots,),
        in_specs=[pl.BlockSpec((1, rows, width), lambda i: (i, 0, 0))] * len(mixed)
        + [pl.BlockSpec(w.shape, lambda i: (0, 0)) for w in flat],
        out_specs=[pl.BlockSpec((1, tok, cols), lambda i: (i, 0, 0))] * 2,
        out_shape=[
            jax.ShapeDtypeStruct((slots, tok, cols), jnp.float32),
            jax.ShapeDtypeStruct((slots, tok, cols), jnp.bfloat16),
        ],
        scratch_shapes=[
            pltpu.VMEM((depth, cols), jnp.bfloat16),
            pltpu.VMEM((rows, depth), jnp.bfloat16),
        ],
        cost_estimate=pl.CostEstimate(
            flops=2 * slots * rows * depth * cols,
            transcendentals=0,
            bytes_accessed=2 * depth * cols + slots * rows * (2 * depth + 3 * cols),
        ),
        name="project",
    )(*mixed, *flat)


def body(latents, timestep, target, qkv_weight, mod_weight, out_weight):
    tok, slots, width = latents.shape
    section = lax.axis_index("section")
    before = jnp.maximum(section - 1, 0)
    own_steps = lax.dynamic_slice_in_dim(timestep, section * slots, slots)
    own_move = lax.dynamic_slice_in_dim(target, section * slots, slots) != section
    prev_steps = lax.dynamic_slice_in_dim(timestep, before * slots, slots)
    prev_move = lax.dynamic_slice_in_dim(target, before * slots, slots) == section
    own_pick = jnp.argmax(own_move)
    prev_pick = jnp.argmax(prev_move)

    outgoing = lax.dynamic_index_in_dim(latents, own_pick, 1, keepdims=False)
    incoming = from_behind(outgoing, "section", 1)
    steps = jnp.concatenate([own_steps, lax.dynamic_slice_in_dim(prev_steps, prev_pick, 1)])
    mods = modulate(steps, mod_weight[0])

    w_own = qkv_weight[0].reshape(width, -1)
    w_peer = swap(w_own, 1)
    w_out = gather_even(out_weight[0], 0)

    sources = [latents[:, l] for l in range(slots)] + [incoming]
    order = [[0], [slots], [1]] if slots == 2 else [[l] for l in range(slots + 1)]
    results = {}
    for group in order:
        values = jnp.stack([sources[l] for l in group]).astype(jnp.float32)
        part = mods[jnp.array(group)]
        hidden = normalize(values, part[:, None, 0], part[:, None, 1]).astype(jnp.bfloat16)
        own, for_peer = project_qkv(gather_even(hidden, 1), w_own, w_peer)
        mixed = attend(own, swap(for_peer, 1), tok)
        mixed = [mixed[i] if m == 0 else swap(mixed[i], m) for i, m in enumerate(chip_masks())]
        proj_own, for_peer = project_out(mixed, w_out)
        proj = proj_own + swap(for_peer, 1).astype(jnp.float32)
        updated = (values + part[:, None, 2] * proj).astype(jnp.bfloat16)
        for i, l in enumerate(group):
            results[l] = updated[i]
    returned = from_behind(results[slots], "section", -1)
    return jnp.stack(
        [jnp.where(own_move[l], returned, results[l]) for l in range(slots)], axis=1
    )


def solution(mesh):
    return jax.shard_map(
        body,
        mesh=mesh,
        in_specs=(
            P("tp", "section", None),
            P(),
            P(),
            P("section", None, None, "tp"),
            P("section", None, None, None),
            P("section", "tp", None),
        ),
        out_specs=P("tp", "section", None),
        check_vma=False,
    )
```
